16 devices in a mesh: dp: 2 (over y, z), sp: 8 (over x, core).
Axes of the slice: x: 4, y: 2, z: 1, core: 2. Of those that a mesh axis runs over, the one named last changes fastest.
The devices are a block of a 4x4x8 slice.
Arguments:
- q: bfloat16 [64, 48, 128], P('dp'), parts along dimension 0
- k: bfloat16 [64, 8192, 4, 128], P('dp', 'sp'), parts along dimension 0
- v: bfloat16 [64, 8192, 4, 128], P('dp', 'sp'), parts along dimension 0
Outputs:
- q: bfloat16 [64, 48, 128], P('dp'), parts along dimension 0
There are 2 independent parts. The reference program is written for one: setup_inputs(seed, part) draws one part's arguments, and reference() takes and returns one part's arrays. A program takes and returns all parts, laid end to end along the dimension named above; each array names one.
All inputs are finite; a program needn't handle non-finite values.
Results may differ from the reference program's by a relative error of at most 0.012.
Values are sent between devices in bfloat16 or wider.
A program may use at most 768 MiB of HBM per device.

```python
import jax
import jax.numpy as jnp

BATCH = 32
CACHE = 8192
HEADS = 48
KV_HEADS = 4
HEAD = 128


def setup_inputs(seed: int = 0, part: int = 0) -> dict:
    kq, kk, kv = (jax.random.fold_in(k, part) for k in jax.random.split(jax.random.key(seed), 3))
    return {
        "q": (3 * jax.random.normal(kq, (BATCH, HEADS, HEAD), jnp.float32)).astype(jnp.bfloat16),
        "k": jax.random.normal(kk, (BATCH, CACHE, KV_HEADS, HEAD), jnp.float32).astype(jnp.bfloat16),
        "v": jax.random.normal(kv, (BATCH, CACHE, KV_HEADS, HEAD), jnp.float32).astype(jnp.bfloat16),
    }


def einsum(form, a, b):
    return jnp.einsum(form, a.astype(jnp.float32), b.astype(jnp.float32))


def reference(q, k, v):
    grouped = q.reshape(BATCH, KV_HEADS, -1, HEAD)
    scores = einsum("bgsd,bugd->bgsu", grouped, k) * HEAD**-0.5
    weights = jax.nn.softmax(scores, -1).astype(jnp.bfloat16)
    return einsum("bgsu,bugd->bgsd", weights, v).astype(jnp.bfloat16).reshape(BATCH, HEADS, HEAD)
```

```python
import functools
import math

import jax
import jax.numpy as jnp
from jax import lax
from jax.experimental import pallas as pl
from jax.experimental.pallas import tpu as pltpu
from jax.sharding import PartitionSpec as P

MESH = pl.DeviceIdType.MESH
SLOTS = 8
LANES = 128
PITCH = 16
AHEAD = 5


def kernel(n, kv, share, scale, q_hbm, k_hbm, v_hbm, o_hbm, q_buf, q_pad, k_buf, v_buf, m_even, m_odd, t_even, t_odd,
           part, stat, got, got_stat, rows, result, q_sem, k_sem, v_sem, send_sem, recv_sem, out_send, out_recv, own_sem):
    sequences, tall, head = k_hbm.shape
    me = lax.axis_index("sp")
    group = tall // 8
    half = tall // 2
    blocks = sequences // n
    power = scale * math.log2(math.e)

    def k_copy(b):
        slot = lax.rem(b, SLOTS)
        return pltpu.make_async_copy(k_hbm.at[b], k_buf.at[slot], k_sem.at[slot])

    def v_copy(b):
        slot = lax.rem(b, SLOTS)
        return pltpu.make_async_copy(v_hbm.at[b], v_buf.at[slot], v_sem.at[slot])

    q_copy = pltpu.make_async_copy(q_hbm, q_buf, q_sem)
    q_copy.start()
    for b in range(SLOTS):
        k_copy(jnp.int32(b)).start()
        v_copy(jnp.int32(b)).start()

    barrier = pltpu.get_barrier_semaphore()
    for d in range(1, n):
        pl.semaphore_signal(barrier, inc=1, device_id={"sp": lax.rem(me + d, n)}, device_id_type=MESH)

    q_copy.wait()

    def spread(b, carry):
        x = q_buf[b].astype(jnp.float32)
        zeros = jnp.zeros((PITCH - share, head), jnp.float32)
        pieces = []
        for h in range(kv):
            pieces += [x[h * share:(h + 1) * share], zeros]
        q_pad[b] = jnp.concatenate(pieces, 0).astype(jnp.bfloat16)
        return carry

    lax.fori_loop(0, sequences, spread, 0)
    pl.semaphore_wait(barrier, n - 1)

    lane = lax.broadcasted_iota(jnp.int32, (8, LANES), 1)
    line = lax.broadcasted_iota(jnp.int32, (8, LANES), 0)
    turn = lax.rem(lane // (2 * PITCH) - lax.rem(line, kv) + kv, kv)
    masks = [turn == w for w in range(kv)]
    lane_row = lax.rem(lax.broadcasted_iota(jnp.int32, (PITCH, LANES), 1), kv)
    keep = [jnp.where(lane_row == h, 1.0, 0.0).astype(jnp.bfloat16) for h in range(kv)]

    def scores(b, m_ref):
        slot = lax.rem(b, SLOTS)
        q = q_pad[b]
        none = jnp.zeros((PITCH, head), jnp.bfloat16)
        for w in range(kv):
            rows_of = []
            for k in range(2 * kv):
                h = (k // 2 - w) % kv
                piece = q[h * PITCH:(h + 1) * PITCH]
                rows_of.append(jnp.concatenate([piece, none] if k % 2 == 0 else [none, piece], 1))
            weights = jnp.concatenate(rows_of, 0)
            keys = jnp.concatenate([k_buf[slot, pl.ds(2 * w * group, group), :], k_buf[slot, pl.ds((2 * w + 1) * group, group), :]], 1)
            s = lax.dot_general(keys, weights, (((1,), (1,)), ((), ())), preferred_element_type=jnp.float32)
            s = s.reshape(group // 8, 8, LANES)
            if w == 0:
                m_ref[...] = s
            else:
                pltpu.store(m_ref, s, mask=jnp.broadcast_to(masks[w][None], s.shape))

    def across(x, op):
        x = op(x, pltpu.roll(x, kv, 0))
        for step in (PITCH, 2 * PITCH, 4 * PITCH):
            x = op(x, pltpu.roll(x, step, 1))
        return x

    def soft(b, m_ref, t_ref):
        s = m_ref[...]
        high = across(jnp.max(s, 0), jnp.maximum)
        p = jnp.exp2((s - high[None]) * power)
        total = across(jnp.sum(p, 0), jnp.add)
        stat[b] = jnp.where(lane < LANES // 2, high, total)
        t_ref[...] = p.reshape(group, LANES).astype(jnp.bfloat16).T

    def mix(b, t_ref):
        slot = lax.rem(b, SLOTS)
        t = t_ref[...]

        def line_of(first):
            columns = []
            for g in range(4):
                w, side = (first + g) // 2, (first + g) % 2
                lines = []
                for h in range(kv):
                    k = 2 * ((h + w) % kv) + side
                    lines.append(t[k * PITCH:(k + 1) * PITCH] * jnp.concatenate([keep[h]] * (group // LANES), 1))
                columns.append(jnp.concatenate(lines, 0))
            return jnp.concatenate(columns, 1)

        left = jnp.concatenate([line_of(0), line_of(4)], 0)
        values = jnp.concatenate([v_buf[slot, pl.ds(0, half), :], v_buf[slot, pl.ds(half, half), :]], 1)
        both = jnp.dot(left, values, preferred_element_type=jnp.float32)
        tall_rows = kv * PITCH
        part[b] = (both[:tall_rows, :head] + both[tall_rows:, head:]).astype(jnp.bfloat16)

    def sends(b):
        i, owner = b // n, lax.rem(b, n)
        to = dict(device_id={"sp": owner}, device_id_type=MESH)
        return (
            pltpu.make_async_remote_copy(src_ref=part.at[b], dst_ref=got.at[i, me], send_sem=send_sem.at[b, 0], recv_sem=recv_sem.at[i, me, 0], **to),
            pltpu.make_async_remote_copy(src_ref=stat.at[b], dst_ref=got_stat.at[i, me], send_sem=send_sem.at[b, 1], recv_sem=recv_sem.at[i, me, 1], **to),
        )

    def send(b):
        @pl.when(lax.rem(b, n) != me)
        def _():
            for copy in sends(b):
                copy.start()

    def arrivals(i, d):
        to = dict(device_id={"sp": d}, device_id_type=MESH)
        return (
            pltpu.make_async_remote_copy(src_ref=part.at[0], dst_ref=got.at[i, d], send_sem=send_sem.at[0, 0], recv_sem=recv_sem.at[i, d, 0], **to),
            pltpu.make_async_remote_copy(src_ref=stat.at[0], dst_ref=got_stat.at[i, d], send_sem=send_sem.at[0, 1], recv_sem=recv_sem.at[i, d, 1], **to),
        )

    def outs(i, d):
        b = i * n + me
        return pltpu.make_async_remote_copy(
            src_ref=result.at[i], dst_ref=o_hbm.at[b], send_sem=out_send.at[i, d], recv_sem=out_recv.at[b],
            device_id={"sp": d}, device_id_type=MESH)

    def own(i):
        return pltpu.make_async_copy(result.at[i], o_hbm.at[i * n + me], own_sem.at[i])

    def together(i):
        b = i * n + me
        got[i, me] = part[b]
        got_stat[i, me] = stat[b]
        for d in range(1, n):
            for copy in arrivals(i, lax.rem(me + d, n)):
                copy.wait_recv()
        stats = [got_stat[i, d] for d in range(n)]
        high = functools.reduce(jnp.maximum, stats)
        factors = [jnp.exp2((x - high) * power) for x in stats]
        total = functools.reduce(jnp.add, [pltpu.roll(x, LANES // 2, 1) * f for x, f in zip(stats, factors)])
        factors = jnp.concatenate([f / total for f in factors] + [jnp.zeros((LANES - 8 * n, LANES), jnp.float32)], 0).T
        for h in range(kv):
            acc = None
            for d in range(n):
                x = got[i, d, pl.ds(h * PITCH, PITCH), :].astype(jnp.float32)
                x = x * factors[:PITCH, 8 * d + h:8 * d + h + 1]
                acc = x if acc is None else acc + x
            rows[pl.ds(h * share, share), :] = acc[:share]
        result[i] = rows[...].astype(jnp.bfloat16)
        own(i).start()
        for d in range(1, n):
            outs(i, lax.rem(me + d, n)).start()

    def step(b, even, a=True, s=True, c=True):
        m_now, m_before = (m_even, m_odd) if even else (m_odd, m_even)
        t_now, t_before = (t_odd, t_even) if even else (t_even, t_odd)
        if a:
            k_copy(b).wait()
        if c:
            v_copy(b - 2).wait()
        if a:
            scores(b, m_now)
        if s:
            soft(b - 1, m_before, t_now)
        if c:
            mix(b - 2, t_before)
        if a:
            @pl.when(b + SLOTS < sequences)
            def _():
                k_copy(b + SLOTS).start()
        if c:
            @pl.when(b - 2 + SLOTS < sequences)
            def _():
                v_copy(b - 2 + SLOTS).start()
            send(b - 2)

    step(jnp.int32(0), True, s=False, c=False)
    step(jnp.int32(1), False, c=False)

    def pair(j, carry):
        b = 2 * j + 2
        step(b, True)

        @pl.when((lax.rem(b - AHEAD - 1, n) == 0) & (b > n + AHEAD))
        def _():
            together((b - AHEAD - 1) // n - 1)

        step(b + 1, False)
        return carry

    lax.fori_loop(0, (sequences - 2) // 2, pair, 0)
    step(jnp.int32(sequences), True, a=False)
    step(jnp.int32(sequences + 1), False, a=False, s=False)
    together(jnp.int32(blocks - 1))

    def finish(b, carry):
        i, owner = b // n, lax.rem(b, n)

        @pl.when(owner != me)
        def _():
            for copy in sends(b):
                copy.wait_send()
            pltpu.make_async_remote_copy(
                src_ref=result.at[i], dst_ref=o_hbm.at[b], send_sem=out_send.at[i, owner], recv_sem=out_recv.at[b],
                device_id={"sp": owner}, device_id_type=MESH).wait_recv()
            outs(i, owner).wait_send()

        @pl.when(owner == me)
        def _():
            own(i).wait()

        return carry

    lax.fori_loop(0, sequences, finish, 0)


def solution(mesh):
    n = mesh.shape["sp"]

    def step(q, k, v):
        sequences, heads, head = q.shape
        tokens, kv = k.shape[1:3]
        share = heads // kv
        tall = tokens * kv
        group = tall // 8
        blocks = sequences // n
        lines = kv * PITCH
        bf16, f32 = jnp.bfloat16, jnp.float32
        anywhere = pl.BlockSpec(memory_space=pl.ANY)
        dma = pltpu.SemaphoreType.DMA
        return pl.pallas_call(
            functools.partial(kernel, n, kv, share, head ** -0.5),
            out_shape=jax.ShapeDtypeStruct(q.shape, bf16),
            in_specs=[anywhere] * 3,
            out_specs=anywhere,
            scratch_shapes=[
                pltpu.VMEM((sequences, heads, head), bf16),
                pltpu.VMEM((sequences, lines, head), bf16),
                pltpu.VMEM((SLOTS, tall, head), bf16),
                pltpu.VMEM((SLOTS, tall, head), bf16),
                pltpu.VMEM((group // 8, 8, LANES), f32),
                pltpu.VMEM((group // 8, 8, LANES), f32),
                pltpu.VMEM((LANES, group), bf16),
                pltpu.VMEM((LANES, group), bf16),
                pltpu.VMEM((sequences, lines, head), bf16),
                pltpu.VMEM((sequences, 8, LANES), f32),
                pltpu.VMEM((blocks, n, lines, head), bf16),
                pltpu.VMEM((blocks, n, 8, LANES), f32),
                pltpu.VMEM((heads, head), f32),
                pltpu.VMEM((blocks, heads, head), bf16),
                dma,
                dma((SLOTS,)),
                dma((SLOTS,)),
                dma((sequences, 2)),
                dma((blocks, n, 2)),
                dma((blocks, n)),
                dma((sequences,)),
                dma((blocks,)),
            ],
            compiler_params=pltpu.CompilerParams(collective_id=0, has_side_effects=True, vmem_limit_bytes=48 * 2 ** 20),
            name="decode",
        )(q, k.reshape(sequences, tall, head), v.reshape(sequences, tall, head))

    return jax.shard_map(
        step,
        mesh=mesh,
        in_specs=(P("dp", None, None), P("dp", "sp", None, None), P("dp", "sp", None, None)),
        out_specs=P("dp", None, None),
        check_vma=False,
    )
```

```python
import functools
import math

import jax
import jax.numpy as jnp
from jax import lax
from jax.experimental import pallas as pl
from jax.experimental.pallas import tpu as pltpu
from jax.sharding import PartitionSpec as P

MESH = pl.DeviceIdType.MESH
PIECES = 4
SLOTS = 8
LANES = 128
PITCH = 16


def kernel(n, kv, share, scale, q_hbm, k_hbm, v_hbm, o_ref, q_buf, k_buf, v_buf, m_even, m_odd, t_even, t_odd,
           part, stat, got, got_stat, late, late_stat, q_sem, k_sem, v_sem, part_send, stat_send, late_send, late_stat_send,
           part_recv, stat_recv, late_recv, late_stat_recv, out_send, out_recv, pair_send, pair_recv):
    sequences, tall, head = k_hbm.shape
    heads = kv * share
    me = lax.axis_index("sp")
    port = lax.rem(me, 2) == 1
    group = tall // 8
    half = tall // 2
    early = sequences - n
    power = scale * math.log2(math.e)

    def k_copy(b):
        slot = lax.rem(b, SLOTS)
        return pltpu.make_async_copy(k_hbm.at[b], k_buf.at[slot], k_sem.at[slot])

    def v_copy(b):
        slot = lax.rem(b, SLOTS)
        return pltpu.make_async_copy(v_hbm.at[b], v_buf.at[slot], v_sem.at[slot])

    q_copy = pltpu.make_async_copy(q_hbm, q_buf, q_sem)
    q_copy.start()
    for i in range(PIECES):
        rows = pl.ds(i * (tall // PIECES), tall // PIECES)
        pltpu.make_async_copy(k_hbm.at[0, rows, :], k_buf.at[0, rows, :], k_sem.at[0]).start()
    k_copy(jnp.int32(1)).start()
    v_copy(jnp.int32(0)).start()

    barrier = pltpu.get_barrier_semaphore()
    for d in range(1, n):
        pl.semaphore_signal(barrier, inc=1, device_id={"sp": lax.rem(me + d, n)}, device_id_type=MESH)
    q_copy.wait()

    lane = lax.broadcasted_iota(jnp.int32, (8, LANES), 1)
    line = lax.broadcasted_iota(jnp.int32, (8, LANES), 0)
    turn = lax.rem(lane // (2 * PITCH) - lax.rem(line, kv) + kv, kv)
    masks = [turn == w for w in range(kv)]
    once = (lax.rem(lane // PITCH, kv) == line)
    lane_row = lax.rem(lax.broadcasted_iota(jnp.int32, (PITCH, LANES), 1), kv)
    keep = [jnp.where(lane_row == h, 1.0, 0.0).astype(jnp.bfloat16) for h in range(kv)]

    def scores(b, m_ref):
        slot = lax.rem(b, SLOTS)
        x = q_buf[b].astype(jnp.float32)
        spare = jnp.zeros((PITCH - share, head), jnp.float32)
        q = [jnp.concatenate([x[h * share:(h + 1) * share], spare], 0).astype(jnp.bfloat16) for h in range(kv)]
        none = jnp.zeros((PITCH, head), jnp.bfloat16)
        for w in range(kv):
            rows_of = []
            for k in range(2 * kv):
                piece = q[(k // 2 - w) % kv]
                rows_of.append(jnp.concatenate([piece, none] if k % 2 == 0 else [none, piece], 1))
            weights = jnp.concatenate(rows_of, 0)
            keys = jnp.concatenate([k_buf[slot, pl.ds(2 * w * group, group), :], k_buf[slot, pl.ds((2 * w + 1) * group, group), :]], 1)
            s = lax.dot_general(keys, weights, (((1,), (1,)), ((), ())), preferred_element_type=jnp.float32)
            s = s.reshape(group // 8, 8, LANES)
            if w == 0:
                m_ref[...] = s
            else:
                pltpu.store(m_ref.at[pl.ds(0, group // 8)], s, mask=jnp.broadcast_to(masks[w][None], s.shape))

    def across(x, op):
        x = op(x, pltpu.roll(x, kv, 0))
        for step in (PITCH, 2 * PITCH, 4 * PITCH):
            x = op(x, pltpu.roll(x, step, 1))
        return x

    def soft(b, m_ref, t_ref):
        s = m_ref[...]
        high = across(jnp.max(s, 0), jnp.maximum)
        p = jnp.exp2((s - high[None]) * power)
        total = across(jnp.sum(p, 0), jnp.add)
        stat[b] = jnp.sum(jnp.where(once, jnp.where(lane < LANES // 2, high, total), 0.0), 0, keepdims=True)
        t_ref[...] = p.reshape(group, LANES).astype(jnp.bfloat16).T

    def compact(x):
        return jnp.concatenate([x[h * PITCH:h * PITCH + share] for h in range(kv)], 0)

    def mix(b, t_ref):
        slot = lax.rem(b, SLOTS)
        t = t_ref[...]

        def line_of(first):
            columns = []
            for g in range(4):
                w, side = (first + g) // 2, (first + g) % 2
                lines = []
                for h in range(kv):
                    k = 2 * ((h + w) % kv) + side
                    lines.append(t[k * PITCH:(k + 1) * PITCH] * jnp.concatenate([keep[h]] * (group // LANES), 1))
                columns.append(jnp.concatenate(lines, 0))
            return jnp.concatenate(columns, 1)

        left = jnp.concatenate([line_of(0), line_of(4)], 0)
        values = jnp.concatenate([v_buf[slot, pl.ds(0, half), :], v_buf[slot, pl.ds(half, half), :]], 1)
        both = jnp.dot(left, values, preferred_element_type=jnp.float32)
        high = kv * PITCH
        part[b] = compact(both[:high, :head] + both[high:, head:]).astype(jnp.bfloat16)

    def remote(src, dst, send_sem, recv_sem, to):
        return pltpu.make_async_remote_copy(src_ref=src, dst_ref=dst, send_sem=send_sem, recv_sem=recv_sem, device_id={"sp": to}, device_id_type=MESH)

    def send_early(b):
        @pl.when((b < early) & (lax.rem(b, n) != me))
        def _():
            k, owner = b // n, lax.rem(b, n)
            remote(stat.at[b], got_stat.at[k, me], stat_send, stat_recv.at[k, me], owner).start()
            remote(part.at[b], got.at[k, me], part_send, part_recv.at[k, me], owner).start()

    def send_late(what, there, send_sem, recv_sem, first, count, group_index):
        for to in range(1, n, 2):
            @pl.when(me != to)
            def _():
                remote(what.at[pl.ds(early + first, count)], there.at[me, pl.ds(first, count)], send_sem, recv_sem.at[group_index, me], jnp.int32(to)).start()

    def late_part(first, count, group_index):
        send_late(part, late, late_send, late_recv, first, count, group_index)

    def late_stats(first, count, group_index):
        send_late(stat, late_stat, late_stat_send, late_stat_recv, first, count, group_index)

    def factors(rows):
        out = []
        for list_of in rows:
            x = jnp.concatenate(list_of, 0)
            f = jnp.exp2((x - jnp.max(x, 0, keepdims=True)) * power)
            total = jnp.sum(pltpu.roll(x, LANES // 2, 1) * f, 0, keepdims=True)
            out.append(f / total)
        if len(rows) * n < LANES:
            out.append(jnp.zeros((LANES - len(rows) * n, LANES), jnp.float32))
        return compact(jnp.concatenate(out, 0).T)

    def put_together(parts, f, i):
        acc = None
        for d, x in enumerate(parts):
            x = x.astype(jnp.float32) * f[:, n * i + d:n * i + d + 1]
            acc = x if acc is None else acc + x
        return acc.astype(jnp.bfloat16)

    def together(k):
        b = k * n + me
        got[k, me] = part[b]
        got_stat[k, me] = stat[b]
        for d in range(1, n):
            other = lax.rem(me + d, n)
            remote(stat.at[0], got_stat.at[k, other], stat_send, stat_recv.at[k, other], other).wait_recv()
            remote(part.at[0], got.at[k, other], part_send, part_recv.at[k, other], other).wait_recv()
        f = factors([[got_stat[k, d] for d in range(n)]])
        o_ref[b] = put_together([got[k, d] for d in range(n)], f, 0)
        for d in range(1, n):
            remote(o_ref.at[b], o_ref.at[b], out_send, out_recv, lax.rem(me + d, n)).start()

    def late_wait(what, there, send_sem, recv_sem, first, count, group_index):
        there[me, pl.ds(first, count)] = what[pl.ds(early + first, count)]
        for d in range(1, n):
            other = lax.rem(me + d, n)
            remote(what.at[pl.ds(0, count)], there.at[other, pl.ds(first, count)], send_sem, recv_sem.at[group_index, other], other).wait_recv()

    def late_factors(first, count):
        return factors([[late_stat[d, first + i] for d in range(n)] for i in range(count)])

    def late_together(first, count, group_index, f, at):
        late_wait(part, late, late_send, late_recv, first, count, group_index)
        for i in range(count):
            o_ref[early + first + i] = put_together([late[d, first + i] for d in range(n)], f, at + i)
        rows = o_ref.at[pl.ds(early + first, count)]
        remote(rows, rows, pair_send, pair_recv, me - 1).start()

    def step(b, even, a=True, s=True, c=True):
        m_now, m_before = (m_even, m_odd) if even else (m_odd, m_even)
        t_now, t_before = (t_odd, t_even) if even else (t_even, t_odd)
        if c:
            if a:
                k_copy(b).wait()
            v_copy(b - 2).wait()
        if a:
            scores(b, m_now)
        if s:
            soft(b - 1, m_before, t_now)
        if c:
            mix(b - 2, t_before)
        if c:
            @pl.when(b + SLOTS < sequences)
            def _():
                k_copy(b + SLOTS).start()

            @pl.when(b - 2 + SLOTS < sequences)
            def _():
                v_copy(b - 2 + SLOTS).start()

    def more(ks, vs):
        for i in ks:
            k_copy(jnp.int32(i)).start()
        for i in vs:
            v_copy(jnp.int32(i)).start()

    k_copy(jnp.int32(0)).wait()
    more((2, 3), (1,))
    step(jnp.int32(0), True, s=False, c=False)
    k_copy(jnp.int32(1)).wait()
    more((4, 5), (2, 3))
    step(jnp.int32(1), False, c=False)
    more((6, 7, 8, 9), (4, 5, 6, 7))
    pl.semaphore_wait(barrier, n - 1)

    def pair(j, carry):
        b = 2 * j + 2

        @pl.when((lax.rem(b, n) == 0) & (b > n))
        def _():
            together(b // n - 2)

        step(b, True)
        send_early(b - 2)
        step(b + 1, False)
        send_early(b - 1)

        @pl.when(b - 2 >= early)
        def _():
            first = b - 2 - early
            late_part(first, 2, first // 2)

        @pl.when(b == early + n // 2 + 2)
        def _():
            late_stats(0, n // 2 + 2, 0)

        return carry

    lax.fori_loop(0, (sequences - 2) // 2, pair, 0)
    step(jnp.int32(sequences), True, a=False)
    late_stats(n - 2, 2, 1)
    late_part(n - 2, 1, n // 2 - 1)
    step(jnp.int32(sequences + 1), False, a=False, s=False)
    late_part(n - 1, 1, n // 2)
    together(jnp.int32(early // n - 1))

    mine = early // n
    others = early - mine

    def sent(what, count, sem):
        remote(what.at[pl.ds(0, count)], what.at[pl.ds(0, count)], sem, pair_recv, lax.rem(me + 1, n)).wait_send()

    def early_waits():
        sent(part, others, part_send)
        sent(stat, others, stat_send)
        sent(o_ref, others, out_send)
        remote(o_ref.at[pl.ds(0, others)], o_ref.at[pl.ds(0, others)], pair_send, out_recv, lax.rem(me + 1, n)).wait_recv()

    @pl.when(port)
    def _():
        late_wait(stat, late_stat, late_stat_send, late_stat_recv, 0, n // 2 + 2, 0)
        f = late_factors(0, n // 2 + 2)
        for i in range(n // 2 - 1):
            late_together(2 * i, 2, i, f, 2 * i)
        late_wait(stat, late_stat, late_stat_send, late_stat_recv, n - 2, 2, 1)
        f = late_factors(n - 2, 2)
        late_together(n - 2, 1, n // 2 - 1, f, 0)
        late_together(n - 1, 1, n // 2, f, 1)
        early_waits()
        sent(part, (n // 2 - 1) * n, late_send)
        sent(stat, (n // 2 - 1) * n, late_stat_send)
        sent(o_ref, n, pair_send)

    @pl.when(jnp.logical_not(port))
    def _():
        early_waits()
        sent(part, n // 2 * n, late_send)
        sent(stat, n // 2 * n, late_stat_send)
        rows = o_ref.at[pl.ds(early, n)]
        remote(rows, rows, pair_send, pair_recv, me + 1).wait_recv()


def solution(mesh):
    n = mesh.shape["sp"]

    def step(q, k, v):
        sequences, heads, head = q.shape
        tokens, kv = k.shape[1:3]
        share = heads // kv
        tall = tokens * kv
        group = tall // 8
        blocks = sequences // n - 1
        bf16, f32 = jnp.bfloat16, jnp.float32
        anywhere = pl.BlockSpec(memory_space=pl.ANY)
        dma = pltpu.SemaphoreType.DMA
        return pl.pallas_call(
            functools.partial(kernel, n, kv, share, head ** -0.5),
            out_shape=jax.ShapeDtypeStruct(q.shape, bf16),
            in_specs=[anywhere] * 3,
            out_specs=pl.BlockSpec(memory_space=pltpu.VMEM),
            scratch_shapes=[
                pltpu.VMEM((sequences, heads, head), bf16),
                pltpu.VMEM((SLOTS, tall, head), bf16),
                pltpu.VMEM((SLOTS, tall, head), bf16),
                pltpu.VMEM((group // 8, 8, LANES), f32),
                pltpu.VMEM((group // 8, 8, LANES), f32),
                pltpu.VMEM((LANES, group), bf16),
                pltpu.VMEM((LANES, group), bf16),
                pltpu.VMEM((sequences, heads, head), bf16),
                pltpu.VMEM((sequences, 1, LANES), f32),
                pltpu.VMEM((blocks, n, heads, head), bf16),
                pltpu.VMEM((blocks, n, 1, LANES), f32),
                pltpu.VMEM((n, n, heads, head), bf16),
                pltpu.VMEM((n, n, 1, LANES), f32),
                dma,
                dma((SLOTS,)),
                dma((SLOTS,)),
                dma,
                dma,
                dma,
                dma,
                dma((blocks, n)),
                dma((blocks, n)),
                dma((n // 2 + 1, n)),
                dma((2, n)),
                dma,
                dma,
                dma,
                dma,
            ],
            compiler_params=pltpu.CompilerParams(collective_id=0, has_side_effects=True, vmem_limit_bytes=56_000_000),
            name="decode",
        )(q, k.reshape(sequences, tall, head), v.reshape(sequences, tall, head))

    return jax.shard_map(
        step,
        mesh=mesh,
        in_specs=(P("dp", None, None), P("dp", "sp", None, None), P("dp", "sp", None, None)),
        out_specs=P("dp", None, None),
        check_vma=False,
    )
```

```python
import functools
import math

import jax
import jax.numpy as jnp
from jax import lax
from jax.experimental import pallas as pl
from jax.experimental.pallas import tpu as pltpu
from jax.sharding import PartitionSpec as P

MESH = pl.DeviceIdType.MESH
PIECES = 4
SLOTS = 8
LANES = 128
PITCH = 16


def kernel(n, kv, share, scale, q_hbm, k_hbm, v_hbm, o_ref, q_buf, k_buf, v_buf, m_even, m_odd, t_even, t_odd,
           part, stat, got, got_stat, late, late_stat, q_sem, k_sem, v_sem, part_send, stat_send, late_send, late_stat_send,
           part_recv, stat_recv, late_recv, late_stat_recv, out_send, out_recv, pair_send, pair_recv):
    sequences, tall, head = k_hbm.shape
    heads = kv * share
    me = lax.axis_index("sp")
    port = lax.rem(me, 2) == 1
    group = tall // 8
    half = tall // 2
    early = sequences - n
    power = scale * math.log2(math.e)
    partner = me + 1 - 2 * lax.rem(me, 2)

    def k_copy(b):
        slot = lax.rem(b, SLOTS)
        return pltpu.make_async_copy(k_hbm.at[b], k_buf.at[slot], k_sem.at[slot])

    def v_copy(b):
        slot = lax.rem(b, SLOTS)
        return pltpu.make_async_copy(v_hbm.at[b], v_buf.at[slot], v_sem.at[slot])

    q_copy = pltpu.make_async_copy(q_hbm, q_buf, q_sem)
    q_copy.start()
    for i in range(PIECES):
        rows = pl.ds(i * (tall // PIECES), tall // PIECES)
        pltpu.make_async_copy(k_hbm.at[0, rows, :], k_buf.at[0, rows, :], k_sem.at[0]).start()
    k_copy(jnp.int32(1)).start()
    v_copy(jnp.int32(0)).start()

    barrier = pltpu.get_barrier_semaphore()
    for d in range(1, n):
        pl.semaphore_signal(barrier, inc=1, device_id={"sp": lax.rem(me + d, n)}, device_id_type=MESH)
    q_copy.wait()

    lane = lax.broadcasted_iota(jnp.int32, (8, LANES), 1)
    line = lax.broadcasted_iota(jnp.int32, (8, LANES), 0)
    turn = lax.rem(lane // (2 * PITCH) - lax.rem(line, kv) + kv, kv)
    masks = [turn == w for w in range(kv)]
    once = (lax.rem(lane // PITCH, kv) == line)
    lane_row = lax.rem(lax.broadcasted_iota(jnp.int32, (PITCH, LANES), 1), kv)
    keep = [jnp.where(lane_row == h, 1.0, 0.0).astype(jnp.bfloat16) for h in range(kv)]

    def scores(b, m_ref):
        slot = lax.rem(b, SLOTS)
        x = q_buf[b].astype(jnp.float32)
        spare = jnp.zeros((PITCH - share, head), jnp.float32)
        q = [jnp.concatenate([x[h * share:(h + 1) * share], spare], 0).astype(jnp.bfloat16) for h in range(kv)]
        none = jnp.zeros((PITCH, head), jnp.bfloat16)
        for w in range(kv):
            rows_of = []
            for k in range(2 * kv):
                piece = q[(k // 2 - w) % kv]
                rows_of.append(jnp.concatenate([piece, none] if k % 2 == 0 else [none, piece], 1))
            weights = jnp.concatenate(rows_of, 0)
            keys = jnp.concatenate([k_buf[slot, pl.ds(2 * w * group, group), :], k_buf[slot, pl.ds((2 * w + 1) * group, group), :]], 1)
            s = lax.dot_general(keys, weights, (((1,), (1,)), ((), ())), preferred_element_type=jnp.float32)
            s = s.reshape(group // 8, 8, LANES)
            if w == 0:
                m_ref[...] = s
            else:
                pltpu.store(m_ref.at[pl.ds(0, group // 8)], s, mask=jnp.broadcast_to(masks[w][None], s.shape))

    def across(x, op):
        x = op(x, pltpu.roll(x, kv, 0))
        for step in (PITCH, 2 * PITCH, 4 * PITCH):
            x = op(x, pltpu.roll(x, step, 1))
        return x

    def soft(b, m_ref, t_ref):
        s = m_ref[...]
        high = across(jnp.max(s, 0), jnp.maximum)
        p = jnp.exp2((s - high[None]) * power)
        total = across(jnp.sum(p, 0), jnp.add)
        stat[b] = jnp.sum(jnp.where(once, jnp.where(lane < LANES // 2, high, total), 0.0), 0, keepdims=True)
        t_ref[...] = p.reshape(group, LANES).astype(jnp.bfloat16).T

    def compact(x):
        return jnp.concatenate([x[h * PITCH:h * PITCH + share] for h in range(kv)], 0)

    def mix(b, t_ref):
        slot = lax.rem(b, SLOTS)
        t = t_ref[...]

        def line_of(first):
            columns = []
            for g in range(4):
                w, side = (first + g) // 2, (first + g) % 2
                lines = []
                for h in range(kv):
                    k = 2 * ((h + w) % kv) + side
                    lines.append(t[k * PITCH:(k + 1) * PITCH] * jnp.concatenate([keep[h]] * (group // LANES), 1))
                columns.append(jnp.concatenate(lines, 0))
            return jnp.concatenate(columns, 1)

        left = jnp.concatenate([line_of(0), line_of(4)], 0)
        values = jnp.concatenate([v_buf[slot, pl.ds(0, half), :], v_buf[slot, pl.ds(half, half), :]], 1)
        both = jnp.dot(left, values, preferred_element_type=jnp.float32)
        high = kv * PITCH
        part[b] = compact(both[:high, :head] + both[high:, head:]).astype(jnp.bfloat16)

    def remote(src, dst, send_sem, recv_sem, to):
        return pltpu.make_async_remote_copy(src_ref=src, dst_ref=dst, send_sem=send_sem, recv_sem=recv_sem, device_id={"sp": to}, device_id_type=MESH)

    def send_early(b):
        owner = jnp.where(b < 2 * n, b // 2, b - 2 * n)
        place = jnp.where(b < 2 * n, lax.rem(b, 2), 2)
        kept = owner == me
        to, at = jnp.where(kept, partner, owner), jnp.where(kept, n, me)
        remote(stat.at[b], got_stat.at[at, place], stat_send, stat_recv.at[place], to).start()
        remote(part.at[b], got.at[at, place], part_send, part_recv.at[place], to).start()

    def send_late(what, there, send_sem, recv_sem, first, count, group_index):
        for r in range(n // 2):
            to = lax.rem(me // 2 + r, n // 2) * 2 + 1
            if r == 0:
                to = jnp.where(port, partner, to)
            remote(what.at[pl.ds(early + first, count)], there.at[me, pl.ds(first, count)], send_sem, recv_sem.at[group_index, me], to).start()

    def late_part(first, count, group_index):
        send_late(part, late, late_send, late_recv, first, count, group_index)

    def late_stats(first, count, group_index):
        send_late(stat, late_stat, late_stat_send, late_stat_recv, first, count, group_index)

    def factors(rows):
        out = []
        for list_of in rows:
            x = jnp.concatenate(list_of, 0)
            f = jnp.exp2((x - jnp.max(x, 0, keepdims=True)) * power)
            total = jnp.sum(pltpu.roll(x, LANES // 2, 1) * f, 0, keepdims=True)
            out.append(f / total)
        if len(rows) * n < LANES:
            out.append(jnp.zeros((LANES - len(rows) * n, LANES), jnp.float32))
        return compact(jnp.concatenate(out, 0).T)

    def put_together(parts, f, i):
        acc = None
        for d, x in enumerate(parts):
            x = x.astype(jnp.float32) * f[:, n * i + d:n * i + d + 1]
            acc = x if acc is None else acc + x
        return acc.astype(jnp.bfloat16)

    def arrived(array, count, sem):
        remote(array.at[pl.ds(0, count)], array.at[pl.ds(0, count)], out_send, sem, partner).wait_recv()

    def together(place, count, first):
        for i in range(count):
            arrived(stat, n, stat_recv.at[place + i])
            arrived(part, n, part_recv.at[place + i])
            got[me, place + i] = part[first + i]
            got_stat[me, place + i] = stat[first + i]
        f = factors([[got_stat[d, place + i] for d in range(n)] for i in range(count)])
        for i in range(count):
            o_ref[first + i] = put_together([got[d, place + i] for d in range(n)], f, i)
        rows = o_ref.at[pl.ds(first, count)]
        for d in range(1, n):
            remote(rows, rows, out_send, out_recv, lax.rem(me + d, n)).start()

    def late_wait(what, there, send_sem, recv_sem, first, count, group_index):
        there[me, pl.ds(first, count)] = what[pl.ds(early + first, count)]
        for d in range(1, n):
            other = lax.rem(me + d, n)
            remote(what.at[pl.ds(0, count)], there.at[other, pl.ds(first, count)], send_sem, recv_sem.at[group_index, other], other).wait_recv()

    def spared(what, there, send_sem, recv_sem, first, count, group_index):
        remote(what.at[pl.ds(0, count)], there.at[partner, pl.ds(first, count)], send_sem, recv_sem.at[group_index, partner], partner).wait_recv()

    def late_factors(first, count):
        return factors([[late_stat[d, first + i] for d in range(n)] for i in range(count)])

    def late_together(first, count, group_index, f, at):
        late_wait(part, late, late_send, late_recv, first, count, group_index)
        for i in range(count):
            o_ref[early + first + i] = put_together([late[d, first + i] for d in range(n)], f, at + i)
        rows = o_ref.at[pl.ds(early + first, count)]
        remote(rows, rows, pair_send, pair_recv, partner).start()

    def step(b, even, a=True, s=True, c=True, more=True, after=None):
        m_now, m_before = (m_even, m_odd) if even else (m_odd, m_even)
        t_now, t_before = (t_odd, t_even) if even else (t_even, t_odd)
        if c:
            if a:
                k_copy(b).wait()
            v_copy(b - 2).wait()
        if a:
            scores(b, m_now)
        if s:
            soft(b - 1, m_before, t_now)
        if c:
            mix(b - 2, t_before)
        if after is not None:
            after()
        if c and more:
            @pl.when(b + SLOTS < sequences)
            def _():
                k_copy(b + SLOTS).start()

            v_copy(b - 2 + SLOTS).start()

    def more(ks, vs):
        for i in ks:
            k_copy(jnp.int32(i)).start()
        for i in vs:
            v_copy(jnp.int32(i)).start()

    k_copy(jnp.int32(0)).wait()
    more((2, 3), (1,))
    step(jnp.int32(0), True, s=False, c=False)
    k_copy(jnp.int32(1)).wait()
    more((4, 5), (2, 3))
    step(jnp.int32(1), False, c=False)
    more((6, 7, 8, 9), (4, 5, 6, 7))
    pl.semaphore_wait(barrier, n - 1)

    def pair(j, carry):
        b = 2 * j + 2

        @pl.when(b == early)
        def _():
            together(0, 2, 2 * me)

        step(b, True, after=lambda: send_early(b - 2))
        step(b + 1, False, after=lambda: send_early(b - 1))
        return carry

    lax.fori_loop(0, early // 2, pair, 0)

    def late_pair(j, carry):
        b = early + 2 + 2 * j
        step(b, True, more=False)
        step(b + 1, False, more=False, after=lambda: late_part(2 * j, 2, j))
        return carry

    lax.fori_loop(0, n // 2 - 1, late_pair, 0)
    late_stats(0, n - 1, 0)
    step(jnp.int32(sequences), True, a=False, more=False, after=lambda: (late_stats(n - 1, 1, 1), late_part(n - 2, 1, n // 2 - 1)))
    step(jnp.int32(sequences + 1), False, a=False, s=False, more=False, after=lambda: late_part(n - 1, 1, n // 2))
    together(2, 1, 2 * n + me)

    mine = early // n
    others = early - mine

    def sent(what, count, sem):
        remote(what.at[pl.ds(0, count)], what.at[pl.ds(0, count)], sem, pair_recv, partner).wait_send()

    def early_waits():
        sent(part, early, part_send)
        sent(stat, early, stat_send)
        sent(o_ref, others, out_send)
        arrived(o_ref, others, out_recv)

    def late_waits():
        for _ in range(n // 2):
            sent(part, n, late_send)
            sent(stat, n, late_stat_send)

    @pl.when(port)
    def _():
        late_wait(stat, late_stat, late_stat_send, late_stat_recv, 0, n - 1, 0)
        f = late_factors(0, n - 1)
        for i in range(n // 2 - 1):
            late_together(2 * i, 2, i, f, 2 * i)
        late_together(n - 2, 1, n // 2 - 1, f, n - 2)
        late_wait(stat, late_stat, late_stat_send, late_stat_recv, n - 1, 1, 1)
        f = late_factors(n - 1, 1)
        late_together(n - 1, 1, n // 2, f, 0)
        early_waits()
        late_waits()
        sent(o_ref, n, pair_send)

    @pl.when(jnp.logical_not(port))
    def _():
        early_waits()
        late_waits()
        for first, count, i in ((0, n - 1, 0), (n - 1, 1, 1)):
            spared(stat, late_stat, late_stat_send, late_stat_recv, first, count, i)
        for i in range(n // 2 - 1):
            spared(part, late, late_send, late_recv, 2 * i, 2, i)
        spared(part, late, late_send, late_recv, n - 2, 1, n // 2 - 1)
        spared(part, late, late_send, late_recv, n - 1, 1, n // 2)
        rows = o_ref.at[pl.ds(early, n)]
        remote(rows, rows, pair_send, pair_recv, partner).wait_recv()


def solution(mesh):
    n = mesh.shape["sp"]

    def step(q, k, v):
        sequences, heads, head = q.shape
        tokens, kv = k.shape[1:3]
        share = heads // kv
        tall = tokens * kv
        group = tall // 8
        bf16, f32 = jnp.bfloat16, jnp.float32
        anywhere = pl.BlockSpec(memory_space=pl.ANY)
        dma = pltpu.SemaphoreType.DMA
        return pl.pallas_call(
            functools.partial(kernel, n, kv, share, head ** -0.5),
            out_shape=jax.ShapeDtypeStruct(q.shape, bf16),
            in_specs=[anywhere] * 3,
            out_specs=pl.BlockSpec(memory_space=pltpu.VMEM),
            scratch_shapes=[
                pltpu.VMEM((sequences, heads, head), bf16),
                pltpu.VMEM((SLOTS, tall, head), bf16),
                pltpu.VMEM((SLOTS, tall, head), bf16),
                pltpu.VMEM((group // 8, 8, LANES), f32),
                pltpu.VMEM((group // 8, 8, LANES), f32),
                pltpu.VMEM((LANES, group), bf16),
                pltpu.VMEM((LANES, group), bf16),
                pltpu.VMEM((sequences, heads, head), bf16),
                pltpu.VMEM((sequences, 1, LANES), f32),
                pltpu.VMEM((n + 1, 3, heads, head), bf16),
                pltpu.VMEM((n + 1, 3, 1, LANES), f32),
                pltpu.VMEM((n, n, heads, head), bf16),
                pltpu.VMEM((n, n, 1, LANES), f32),
                dma,
                dma((SLOTS,)),
                dma((SLOTS,)),
                dma,
                dma,
                dma,
                dma,
                dma((3,)),
                dma((3,)),
                dma((n // 2 + 1, n)),
                dma((2, n)),
                dma,
                dma,
                dma,
                dma,
            ],
            compiler_params=pltpu.CompilerParams(collective_id=0, has_side_effects=True, vmem_limit_bytes=56_000_000),
            name="decode",
        )(q, k.reshape(sequences, tall, head), v.reshape(sequences, tall, head))

    return jax.shard_map(
        step,
        mesh=mesh,
        in_specs=(P("dp", None, None), P("dp", "sp", None, None), P("dp", "sp", None, None)),
        out_specs=P("dp", None, None),
        check_vma=False,
    )
```

```python
import functools
import math

import jax
import jax.numpy as jnp
from jax import lax
from jax.experimental import pallas as pl
from jax.experimental.pallas import tpu as pltpu
from jax.sharding import PartitionSpec as P

MESH = pl.DeviceIdType.MESH
PIECES = 4
LAG = 8
SLOTS = 8
LANES = 128
PITCH = 16


def kernel(n, kv, share, scale, q_hbm, k_hbm, v_hbm, o_ref, q_buf, k_buf, v_buf, m_even, m_odd, t_even, t_odd,
           part, stat, got, got_stat, late, late_stat, q_sem, k_sem, v_sem, part_send, stat_send, late_send, late_stat_send,
           part_recv, stat_recv, late_recv, late_stat_recv, out_send, out_recv, hand_send, hand_recv, pair_send, pair_recv):
    sequences, tall, head = k_hbm.shape
    heads = kv * share
    me = lax.axis_index("sp")
    port = lax.rem(me, 2) == 1
    group = tall // 8
    half = tall // 2
    early = sequences - n
    power = scale * math.log2(math.e)
    partner = me + 1 - 2 * lax.rem(me, 2)

    def k_copy(b):
        slot = lax.rem(b, SLOTS)
        return pltpu.make_async_copy(k_hbm.at[b], k_buf.at[slot], k_sem.at[slot])

    def v_copy(b):
        slot = lax.rem(b, SLOTS)
        return pltpu.make_async_copy(v_hbm.at[b], v_buf.at[slot], v_sem.at[slot])

    q_copy = pltpu.make_async_copy(q_hbm, q_buf, q_sem)
    q_copy.start()
    for i in range(PIECES):
        rows = pl.ds(i * (tall // PIECES), tall // PIECES)
        pltpu.make_async_copy(k_hbm.at[0, rows, :], k_buf.at[0, rows, :], k_sem.at[0]).start()
    k_copy(jnp.int32(1)).start()
    v_copy(jnp.int32(0)).start()

    barrier = pltpu.get_barrier_semaphore()
    for d in range(1, n):
        pl.semaphore_signal(barrier, inc=1, device_id={"sp": lax.rem(me + d, n)}, device_id_type=MESH)
    q_copy.wait()

    lane = lax.broadcasted_iota(jnp.int32, (8, LANES), 1)
    line = lax.broadcasted_iota(jnp.int32, (8, LANES), 0)
    turn = lax.rem(lane // (2 * PITCH) - lax.rem(line, kv) + kv, kv)
    masks = [turn == w for w in range(kv)]
    once = (lax.rem(lane // PITCH, kv) == line)
    lane_row = lax.rem(lax.broadcasted_iota(jnp.int32, (PITCH, LANES), 1), kv)
    keep = [jnp.where(lane_row == h, 1.0, 0.0).astype(jnp.bfloat16) for h in range(kv)]

    def scores(b, m_ref):
        slot = lax.rem(b, SLOTS)
        x = q_buf[b].astype(jnp.float32)
        spare = jnp.zeros((PITCH - share, head), jnp.float32)
        q = [jnp.concatenate([x[h * share:(h + 1) * share], spare], 0).astype(jnp.bfloat16) for h in range(kv)]
        none = jnp.zeros((PITCH, head), jnp.bfloat16)
        for w in range(kv):
            rows_of = []
            for k in range(2 * kv):
                piece = q[(k // 2 - w) % kv]
                rows_of.append(jnp.concatenate([piece, none] if k % 2 == 0 else [none, piece], 1))
            weights = jnp.concatenate(rows_of, 0)
            keys = jnp.concatenate([k_buf[slot, pl.ds(2 * w * group, group), :], k_buf[slot, pl.ds((2 * w + 1) * group, group), :]], 1)
            s = lax.dot_general(keys, weights, (((1,), (1,)), ((), ())), preferred_element_type=jnp.float32)
            s = s.reshape(group // 8, 8, LANES)
            if w == 0:
                m_ref[...] = s
            else:
                pltpu.store(m_ref.at[pl.ds(0, group // 8)], s, mask=jnp.broadcast_to(masks[w][None], s.shape))

    def across(x, op):
        x = op(x, pltpu.roll(x, kv, 0))
        for step in (PITCH, 2 * PITCH, 4 * PITCH):
            x = op(x, pltpu.roll(x, step, 1))
        return x

    def soft(b, m_ref, t_ref):
        s = m_ref[...]
        high = across(jnp.max(s, 0), jnp.maximum)
        p = jnp.exp2((s - high[None]) * power)
        total = across(jnp.sum(p, 0), jnp.add)
        stat[b] = jnp.sum(jnp.where(once, jnp.where(lane < LANES // 2, high, total), 0.0), 0, keepdims=True)
        t_ref[...] = p.reshape(group, LANES).astype(jnp.bfloat16).T

    def compact(x):
        return jnp.concatenate([x[h * PITCH:h * PITCH + share] for h in range(kv)], 0)

    def mix(b, t_ref):
        slot = lax.rem(b, SLOTS)
        t = t_ref[...]

        def line_of(first):
            columns = []
            for g in range(4):
                w, side = (first + g) // 2, (first + g) % 2
                lines = []
                for h in range(kv):
                    k = 2 * ((h + w) % kv) + side
                    lines.append(t[k * PITCH:(k + 1) * PITCH] * jnp.concatenate([keep[h]] * (group // LANES), 1))
                columns.append(jnp.concatenate(lines, 0))
            return jnp.concatenate(columns, 1)

        left = jnp.concatenate([line_of(0), line_of(4)], 0)
        values = jnp.concatenate([v_buf[slot, pl.ds(0, half), :], v_buf[slot, pl.ds(half, half), :]], 1)
        both = jnp.dot(left, values, preferred_element_type=jnp.float32)
        high = kv * PITCH
        part[b] = compact(both[:high, :head] + both[high:, head:]).astype(jnp.bfloat16)

    def remote(src, dst, send_sem, recv_sem, to):
        return pltpu.make_async_remote_copy(src_ref=src, dst_ref=dst, send_sem=send_sem, recv_sem=recv_sem, device_id={"sp": to}, device_id_type=MESH)

    def send_early(b):
        k = b // n
        owner = lax.rem(b, n) + jnp.where(k == 1, 0, 1)
        kept = owner == me
        to, at = jnp.where(kept, partner, owner), jnp.where(kept, n, me)
        pair_of, places = pl.ds(b, 2), pl.ds(2 * k, 2)
        remote(stat.at[pair_of], got_stat.at[at, places], stat_send, stat_recv.at[k], to).start()
        remote(part.at[pair_of], got.at[at, places], part_send, part_recv.at[k], to).start()

    def send_late(what, there, send_sem, recv_sem, first, count, group_index):
        for r in range(n // 2):
            to = lax.rem(me // 2 + r, n // 2) * 2 + 1
            if r == 0:
                to = jnp.where(port, partner, to)
            remote(what.at[pl.ds(early + first, count)], there.at[me, pl.ds(first, count)], send_sem, recv_sem.at[group_index, me], to).start()

    def late_part(first, count, group_index):
        send_late(part, late, late_send, late_recv, first, count, group_index)

    def late_stats(first, count, group_index):
        send_late(stat, late_stat, late_stat_send, late_stat_recv, first, count, group_index)

    def factors(rows):
        out = []
        for list_of in rows:
            x = jnp.concatenate(list_of, 0)
            f = jnp.exp2((x - jnp.max(x, 0, keepdims=True)) * power)
            total = jnp.sum(pltpu.roll(x, LANES // 2, 1) * f, 0, keepdims=True)
            out.append(f / total)
        if len(rows) * n < LANES:
            out.append(jnp.zeros((LANES - len(rows) * n, LANES), jnp.float32))
        return compact(jnp.concatenate(out, 0).T)

    def put_together(parts, f, i):
        acc = None
        for d, x in enumerate(parts):
            x = x.astype(jnp.float32) * f[:, n * i + d:n * i + d + 1]
            acc = x if acc is None else acc + x
        return acc.astype(jnp.bfloat16)

    def arrived(array, count, sem):
        remote(array.at[pl.ds(0, count)], array.at[pl.ds(0, count)], out_send, sem, partner).wait_recv()

    def come(k, count):
        arrived(stat, count, stat_recv.at[k])
        arrived(part, count, part_recv.at[k])

    def together(k):
        first = k * n + me - lax.rem(me, 2)
        places = range(2 * k, 2 * k + 2)
        come(k, 2 * (n - 1))
        for i, place in enumerate(places):
            got[me, place] = part[first + i]
            got_stat[me, place] = stat[first + i]
        f = factors([[got_stat[d, place] for d in range(n)] for place in places])
        for i, place in enumerate(places):
            o_ref[first + i] = put_together([got[d, place] for d in range(n)], f, i)
        rows = o_ref.at[pl.ds(first, 2)]
        for d in range(2, n, 2):
            remote(rows, rows, out_send, out_recv.at[k], lax.rem(me + d, n)).start()

    def hand_on(k):
        arrived(o_ref, n - 2, out_recv.at[k])
        rows = o_ref.at[pl.ds(k * n, n)]
        remote(rows, rows, hand_send, hand_recv, partner).start()

    def late_wait(what, there, send_sem, recv_sem, first, count, group_index):
        there[me, pl.ds(first, count)] = what[pl.ds(early + first, count)]
        for d in range(1, n):
            other = lax.rem(me + d, n)
            remote(what.at[pl.ds(0, count)], there.at[other, pl.ds(first, count)], send_sem, recv_sem.at[group_index, other], other).wait_recv()

    def spared(what, there, send_sem, recv_sem, first, count, group_index):
        remote(what.at[pl.ds(0, count)], there.at[partner, pl.ds(first, count)], send_sem, recv_sem.at[group_index, partner], partner).wait_recv()

    def late_factors(first, count):
        return factors([[late_stat[d, first + i] for d in range(n)] for i in range(count)])

    def late_together(first, count, group_index, f, at):
        late_wait(part, late, late_send, late_recv, first, count, group_index)
        for i in range(count):
            o_ref[early + first + i] = put_together([late[d, first + i] for d in range(n)], f, at + i)
        rows = o_ref.at[pl.ds(early + first, count)]
        remote(rows, rows, pair_send, pair_recv, partner).start()

    def step(b, even, a=True, s=True, c=True, more=True, between=None, after=None):
        m_now, m_before = (m_even, m_odd) if even else (m_odd, m_even)
        t_now, t_before = (t_odd, t_even) if even else (t_even, t_odd)
        if c:
            if a:
                k_copy(b).wait()
            v_copy(b - 2).wait()
        if a:
            scores(b, m_now)
        if s:
            soft(b - 1, m_before, t_now)
        if between is not None:
            between()
        if c:
            mix(b - 2, t_before)
        if after is not None:
            after()
        if c and more:
            @pl.when(b + SLOTS < sequences)
            def _():
                k_copy(b + SLOTS).start()

            v_copy(b - 2 + SLOTS).start()

    def more(ks, vs):
        for i in ks:
            k_copy(jnp.int32(i)).start()
        for i in vs:
            v_copy(jnp.int32(i)).start()

    k_copy(jnp.int32(0)).wait()
    more((2, 3), (1,))
    step(jnp.int32(0), True, s=False, c=False)
    k_copy(jnp.int32(1)).wait()
    more((4, 5), (2, 3))
    step(jnp.int32(1), False, c=False)
    more((6, 7, 8, 9), (4, 5, 6, 7))
    pl.semaphore_wait(barrier, n - 1)

    def pair(j, carry):
        b = 2 * j + 2

        @pl.when(port & (b == n + LAG))
        def _():
            together(0)

        @pl.when(jnp.logical_not(port) & (b == 2 * n + LAG))
        def _():
            together(1)

        step(b, True)
        step(b + 1, False, after=lambda: send_early(b - 2))
        return carry

    lax.fori_loop(0, early // 2, pair, 0)

    b = jnp.int32(early + 2)
    for i in range(n - 2):
        between = (lambda: late_stats(0, n - 1, 0)) if i == n - 3 else None
        after = (lambda: late_part(i - 1, 2, i // 2)) if i % 2 == 1 else None
        step(b + i, i % 2 == 0, more=False, between=between, after=after)
    step(jnp.int32(sequences), True, a=False, more=False, between=lambda: late_stats(n - 1, 1, 1), after=lambda: late_part(n - 2, 1, n // 2 - 1))
    step(jnp.int32(sequences + 1), False, a=False, s=False, more=False, after=lambda: late_part(n - 1, 1, n // 2))


    def sent(what, count, sem):
        remote(what.at[pl.ds(0, count)], what.at[pl.ds(0, count)], sem, pair_recv, partner).wait_send()

    def early_waits(handed):
        sent(part, early, part_send)
        sent(stat, early, stat_send)
        sent(o_ref, n - 2, out_send)
        sent(o_ref, n, hand_send)
        arrived(o_ref, handed, hand_recv)

    def late_waits():
        for _ in range(n // 2):
            sent(part, n, late_send)
            sent(stat, n, late_stat_send)

    @pl.when(port)
    def _():
        hand_on(0)
        come(1, 2)
        together(2)
        late_wait(stat, late_stat, late_stat_send, late_stat_recv, 0, n - 1, 0)
        f = late_factors(0, n - 1)
        for i in range(n // 2 - 1):
            late_together(2 * i, 2, i, f, 2 * i)
        late_together(n - 2, 1, n // 2 - 1, f, n - 2)
        late_wait(stat, late_stat, late_stat_send, late_stat_recv, n - 1, 1, 1)
        f = late_factors(n - 1, 1)
        late_together(n - 1, 1, n // 2, f, 0)
        hand_on(2)
        early_waits(n)
        late_waits()
        sent(o_ref, n - 2, out_send)
        sent(o_ref, n, hand_send)
        sent(o_ref, n, pair_send)

    @pl.when(jnp.logical_not(port))
    def _():
        hand_on(1)
        come(0, 2)
        come(2, 2)
        late_waits()
        for first, count, i in ((0, n - 1, 0), (n - 1, 1, 1)):
            spared(stat, late_stat, late_stat_send, late_stat_recv, first, count, i)
        for i in range(n // 2 - 1):
            spared(part, late, late_send, late_recv, 2 * i, 2, i)
        spared(part, late, late_send, late_recv, n - 2, 1, n // 2 - 1)
        spared(part, late, late_send, late_recv, n - 1, 1, n // 2)
        early_waits(2 * n)
        arrived(o_ref, n, pair_recv)


def solution(mesh):
    n = mesh.shape["sp"]

    def step(q, k, v):
        sequences, heads, head = q.shape
        tokens, kv = k.shape[1:3]
        share = heads // kv
        tall = tokens * kv
        group = tall // 8
        bf16, f32 = jnp.bfloat16, jnp.float32
        anywhere = pl.BlockSpec(memory_space=pl.ANY)
        dma = pltpu.SemaphoreType.DMA
        return pl.pallas_call(
            functools.partial(kernel, n, kv, share, head ** -0.5),
            out_shape=jax.ShapeDtypeStruct(q.shape, bf16),
            in_specs=[anywhere] * 3,
            out_specs=pl.BlockSpec(memory_space=pltpu.VMEM),
            scratch_shapes=[
                pltpu.VMEM((sequences, heads, head), bf16),
                pltpu.VMEM((SLOTS, tall, head), bf16),
                pltpu.VMEM((SLOTS, tall, head), bf16),
                pltpu.VMEM((group // 8, 8, LANES), f32),
                pltpu.VMEM((group // 8, 8, LANES), f32),
                pltpu.VMEM((LANES, group), bf16),
                pltpu.VMEM((LANES, group), bf16),
                pltpu.VMEM((sequences, heads, head), bf16),
                pltpu.VMEM((sequences, 1, LANES), f32),
                pltpu.VMEM((n + 1, 6, heads, head), bf16),
                pltpu.VMEM((n + 1, 6, 1, LANES), f32),
                pltpu.VMEM((n, n, heads, head), bf16),
                pltpu.VMEM((n, n, 1, LANES), f32),
                dma,
                dma((SLOTS,)),
                dma((SLOTS,)),
                dma,
                dma,
                dma,
                dma,
                dma((3,)),
                dma((3,)),
                dma((n // 2 + 1, n)),
                dma((2, n)),
                dma,
                dma((3,)),
                dma,
                dma,
                dma,
                dma,
            ],
            compiler_params=pltpu.CompilerParams(collective_id=0, has_side_effects=True, vmem_limit_bytes=56_000_000),
            name="decode",
        )(q, k.reshape(sequences, tall, head), v.reshape(sequences, tall, head))

    return jax.shard_map(
        step,
        mesh=mesh,
        in_specs=(P("dp", None, None), P("dp", "sp", None, None), P("dp", "sp", None, None)),
        out_specs=P("dp", None, None),
        check_vma=False,
    )
```

```python
import functools
import math

import jax
import jax.numpy as jnp
from jax import lax
from jax.experimental import pallas as pl
from jax.experimental.pallas import tpu as pltpu
from jax.sharding import PartitionSpec as P

MESH = pl.DeviceIdType.MESH
PIECES = 4
LAG = 8
SLOTS = 8
LANES = 128
PITCH = 16


def kernel(n, kv, share, scale, q_hbm, k_hbm, v_hbm, o_ref, q_buf, k_buf, v_buf, m_even, m_odd, t_even, t_odd,
           part, stat, got, got_stat, late, late_stat, q_sem, k_sem, v_sem, part_send, stat_send, late_send, late_stat_send,
           part_recv, stat_recv, late_recv, late_stat_recv, out_send, out_recv, hand_send, hand_recv, pair_send, pair_recv):
    sequences, tall, head = k_hbm.shape
    heads = kv * share
    me = lax.axis_index("sp")
    port = lax.rem(me, 2) == 1
    group = tall // 8
    half = tall // 2
    early = sequences - n
    power = scale * math.log2(math.e)
    partner = me + 1 - 2 * lax.rem(me, 2)

    def k_copy(b):
        slot = lax.rem(b, SLOTS)
        return pltpu.make_async_copy(k_hbm.at[b], k_buf.at[slot], k_sem.at[slot])

    def v_copy(b):
        slot = lax.rem(b, SLOTS)
        return pltpu.make_async_copy(v_hbm.at[b], v_buf.at[slot], v_sem.at[slot])

    q_copy = pltpu.make_async_copy(q_hbm, q_buf, q_sem)
    q_copy.start()
    for i in range(PIECES):
        rows = pl.ds(i * (tall // PIECES), tall // PIECES)
        pltpu.make_async_copy(k_hbm.at[0, rows, :], k_buf.at[0, rows, :], k_sem.at[0]).start()
    k_copy(jnp.int32(1)).start()
    v_copy(jnp.int32(0)).start()

    barrier = pltpu.get_barrier_semaphore()
    for d in range(1, n):
        pl.semaphore_signal(barrier, inc=1, device_id={"sp": lax.rem(me + d, n)}, device_id_type=MESH)
    q_copy.wait()

    lane = lax.broadcasted_iota(jnp.int32, (8, LANES), 1)
    line = lax.broadcasted_iota(jnp.int32, (8, LANES), 0)
    turn = lax.rem(lane // (2 * PITCH) - lax.rem(line, kv) + kv, kv)
    masks = [turn == w for w in range(kv)]
    once = (lax.rem(lane // PITCH, kv) == line)
    lane_row = lax.rem(lax.broadcasted_iota(jnp.int32, (PITCH, LANES), 1), kv)
    keep = [jnp.where(lane_row == h, 1.0, 0.0).astype(jnp.bfloat16) for h in range(kv)]

    def abreast(x):
        x = x.reshape(x.shape[0] // (2 * PITCH), 2, PITCH, head)
        return jnp.concatenate([x[:, side].reshape(-1, head) for side in range(2)], 1)

    def scores(b, m_ref):
        slot = lax.rem(b, SLOTS)
        x = q_buf[b].astype(jnp.float32)
        spare = jnp.zeros((PITCH - share, head), jnp.float32)
        q = [jnp.concatenate([x[h * share:(h + 1) * share], spare], 0).astype(jnp.bfloat16) for h in range(kv)]
        none = jnp.zeros((PITCH, head), jnp.bfloat16)
        for w in range(kv):
            rows_of = []
            for k in range(2 * kv):
                piece = q[(k // 2 - w) % kv]
                rows_of.append(jnp.concatenate([piece, none] if k % 2 == 0 else [none, piece], 1))
            weights = jnp.concatenate(rows_of, 0)
            keys = abreast(k_buf[slot, pl.ds(2 * w * group, 2 * group), :])
            s = lax.dot_general(keys, weights, (((1,), (1,)), ((), ())), preferred_element_type=jnp.float32)
            s = s.reshape(group // 8, 8, LANES)
            if w == 0:
                m_ref[...] = s
            else:
                pltpu.store(m_ref.at[pl.ds(0, group // 8)], s, mask=jnp.broadcast_to(masks[w][None], s.shape))

    def across(x, op):
        x = op(x, pltpu.roll(x, kv, 0))
        for step in (PITCH, 2 * PITCH, 4 * PITCH):
            x = op(x, pltpu.roll(x, step, 1))
        return x

    def soft(b, m_ref, t_ref):
        s = m_ref[...]
        high = across(jnp.max(s, 0), jnp.maximum)
        p = jnp.exp2((s - high[None]) * power)
        total = across(jnp.sum(p, 0), jnp.add)
        stat[b] = jnp.sum(jnp.where(once, jnp.where(lane < LANES // 2, high, total), 0.0), 0, keepdims=True)
        t_ref[...] = p.reshape(group, LANES).astype(jnp.bfloat16).T

    def compact(x):
        return jnp.concatenate([x[h * PITCH:h * PITCH + share] for h in range(kv)], 0)

    def mix(b, t_ref):
        slot = lax.rem(b, SLOTS)
        t = t_ref[...]

        def line_of(side):
            columns = []
            for w in range(kv):
                lines = []
                for h in range(kv):
                    k = 2 * ((h + w) % kv) + side
                    lines.append(t[k * PITCH:(k + 1) * PITCH] * jnp.concatenate([keep[h]] * (group // LANES), 1))
                columns.append(jnp.concatenate(lines, 0))
            return jnp.concatenate(columns, 1)

        left = jnp.concatenate([line_of(0), line_of(1)], 0)
        values = abreast(v_buf[slot])
        both = jnp.dot(left, values, preferred_element_type=jnp.float32)
        high = kv * PITCH
        part[b] = compact(both[:high, :head] + both[high:, head:]).astype(jnp.bfloat16)

    def remote(src, dst, send_sem, recv_sem, to):
        return pltpu.make_async_remote_copy(src_ref=src, dst_ref=dst, send_sem=send_sem, recv_sem=recv_sem, device_id={"sp": to}, device_id_type=MESH)

    def send_early(b):
        k = b // n
        owner = lax.rem(b, n) + jnp.where(k == 1, 0, 1)
        kept = owner == me
        to, at = jnp.where(kept, partner, owner), jnp.where(kept, n, me)
        pair_of, places = pl.ds(b, 2), pl.ds(2 * k, 2)
        remote(stat.at[pair_of], got_stat.at[at, places], stat_send, stat_recv.at[k], to).start()
        remote(part.at[pair_of], got.at[at, places], part_send, part_recv.at[k], to).start()

    def send_late(what, there, send_sem, recv_sem, first, count, group_index):
        for r in range(n // 2):
            to = lax.rem(me // 2 + r, n // 2) * 2 + 1
            if r == 0:
                to = jnp.where(port, partner, to)
            remote(what.at[pl.ds(early + first, count)], there.at[me, pl.ds(first, count)], send_sem, recv_sem.at[group_index, me], to).start()

    def late_part(first, count, group_index):
        send_late(part, late, late_send, late_recv, first, count, group_index)

    def late_stats(first, count, group_index):
        send_late(stat, late_stat, late_stat_send, late_stat_recv, first, count, group_index)

    def factors(rows):
        out = []
        for list_of in rows:
            x = jnp.concatenate(list_of, 0)
            f = jnp.exp2((x - jnp.max(x, 0, keepdims=True)) * power)
            total = jnp.sum(pltpu.roll(x, LANES // 2, 1) * f, 0, keepdims=True)
            out.append(f / total)
        if len(rows) * n < LANES:
            out.append(jnp.zeros((LANES - len(rows) * n, LANES), jnp.float32))
        return compact(jnp.concatenate(out, 0).T)

    def put_together(parts, f, i):
        acc = None
        for d, x in enumerate(parts):
            x = x.astype(jnp.float32) * f[:, n * i + d:n * i + d + 1]
            acc = x if acc is None else acc + x
        return acc.astype(jnp.bfloat16)

    def arrived(array, count, sem):
        remote(array.at[pl.ds(0, count)], array.at[pl.ds(0, count)], out_send, sem, partner).wait_recv()

    def come(k, count):
        arrived(stat, count, stat_recv.at[k])
        arrived(part, count, part_recv.at[k])

    def together(k):
        first = k * n + me - lax.rem(me, 2)
        places = range(2 * k, 2 * k + 2)
        come(k, 2 * (n - 1))
        for i, place in enumerate(places):
            got[me, place] = part[first + i]
            got_stat[me, place] = stat[first + i]
        f = factors([[got_stat[d, place] for d in range(n)] for place in places])
        for i, place in enumerate(places):
            o_ref[first + i] = put_together([got[d, place] for d in range(n)], f, i)
        rows = o_ref.at[pl.ds(first, 2)]
        for d in range(2, n, 2):
            remote(rows, rows, out_send, out_recv.at[k], lax.rem(me + d, n)).start()

    def hand_on(k):
        arrived(o_ref, n - 2, out_recv.at[k])
        rows = o_ref.at[pl.ds(k * n, n)]
        remote(rows, rows, hand_send, hand_recv, partner).start()

    def late_wait(what, there, send_sem, recv_sem, first, count, group_index):
        there[me, pl.ds(first, count)] = what[pl.ds(early + first, count)]
        for d in range(1, n):
            other = lax.rem(me + d, n)
            remote(what.at[pl.ds(0, count)], there.at[other, pl.ds(first, count)], send_sem, recv_sem.at[group_index, other], other).wait_recv()

    def spared(what, there, send_sem, recv_sem, first, count, group_index):
        remote(what.at[pl.ds(0, count)], there.at[partner, pl.ds(first, count)], send_sem, recv_sem.at[group_index, partner], partner).wait_recv()

    def late_factors(first, count):
        return factors([[late_stat[d, first + i] for d in range(n)] for i in range(count)])

    def late_together(first, count, group_index, f, at):
        late_wait(part, late, late_send, late_recv, first, count, group_index)
        for i in range(count):
            o_ref[early + first + i] = put_together([late[d, first + i] for d in range(n)], f, at + i)
        rows = o_ref.at[pl.ds(early + first, count)]
        remote(rows, rows, pair_send, pair_recv, partner).start()

    def step(b, even, a=True, s=True, c=True, more=True, between=None, after=None):
        m_now, m_before = (m_even, m_odd) if even else (m_odd, m_even)
        t_now, t_before = (t_odd, t_even) if even else (t_even, t_odd)
        if c:
            if a:
                k_copy(b).wait()
            v_copy(b - 2).wait()
        if a:
            scores(b, m_now)
        if s:
            soft(b - 1, m_before, t_now)
        if between is not None:
            between()
        if c:
            mix(b - 2, t_before)
        if after is not None:
            after()
        if c and more:
            @pl.when(b + SLOTS < sequences)
            def _():
                k_copy(b + SLOTS).start()

            v_copy(b - 2 + SLOTS).start()

    def more(ks, vs):
        for i in ks:
            k_copy(jnp.int32(i)).start()
        for i in vs:
            v_copy(jnp.int32(i)).start()

    k_copy(jnp.int32(0)).wait()
    more((2, 3), (1,))
    step(jnp.int32(0), True, s=False, c=False)
    k_copy(jnp.int32(1)).wait()
    more((4, 5), (2, 3))
    step(jnp.int32(1), False, c=False)
    more((6, 7, 8, 9), (4, 5, 6, 7))
    pl.semaphore_wait(barrier, n - 1)

    def pair(j, carry):
        b = 2 * j + 2

        @pl.when(port & (b == n + LAG))
        def _():
            together(0)

        @pl.when(jnp.logical_not(port) & (b == 2 * n + LAG))
        def _():
            together(1)

        step(b, True)
        step(b + 1, False, after=lambda: send_early(b - 2))
        return carry

    lax.fori_loop(0, early // 2, pair, 0)

    b = jnp.int32(early + 2)
    for i in range(n - 2):
        between = (lambda: late_stats(0, n - 1, 0)) if i == n - 3 else None
        after = (lambda: late_part(i - 1, 2, i // 2)) if i % 2 == 1 else None
        step(b + i, i % 2 == 0, more=False, between=between, after=after)
    step(jnp.int32(sequences), True, a=False, more=False, between=lambda: late_stats(n - 1, 1, 1), after=lambda: late_part(n - 2, 1, n // 2 - 1))
    step(jnp.int32(sequences + 1), False, a=False, s=False, more=False, after=lambda: late_part(n - 1, 1, n // 2))


    def sent(what, count, sem):
        remote(what.at[pl.ds(0, count)], what.at[pl.ds(0, count)], sem, pair_recv, partner).wait_send()

    def early_waits(handed):
        sent(part, early, part_send)
        sent(stat, early, stat_send)
        sent(o_ref, n - 2, out_send)
        sent(o_ref, n, hand_send)
        arrived(o_ref, handed, hand_recv)

    def late_waits():
        for _ in range(n // 2):
            sent(part, n, late_send)
            sent(stat, n, late_stat_send)

    @pl.when(port)
    def _():
        hand_on(0)
        come(1, 2)
        together(2)
        late_wait(stat, late_stat, late_stat_send, late_stat_recv, 0, n - 1, 0)
        f = late_factors(0, n - 1)
        for i in range(n // 2 - 1):
            late_together(2 * i, 2, i, f, 2 * i)
        late_together(n - 2, 1, n // 2 - 1, f, n - 2)
        late_wait(stat, late_stat, late_stat_send, late_stat_recv, n - 1, 1, 1)
        f = late_factors(n - 1, 1)
        late_together(n - 1, 1, n // 2, f, 0)
        hand_on(2)
        early_waits(n)
        late_waits()
        sent(o_ref, n - 2, out_send)
        sent(o_ref, n, hand_send)
        sent(o_ref, n, pair_send)

    @pl.when(jnp.logical_not(port))
    def _():
        hand_on(1)
        come(0, 2)
        come(2, 2)
        late_waits()
        for first, count, i in ((0, n - 1, 0), (n - 1, 1, 1)):
            spared(stat, late_stat, late_stat_send, late_stat_recv, first, count, i)
        for i in range(n // 2 - 1):
            spared(part, late, late_send, late_recv, 2 * i, 2, i)
        spared(part, late, late_send, late_recv, n - 2, 1, n // 2 - 1)
        spared(part, late, late_send, late_recv, n - 1, 1, n // 2)
        early_waits(2 * n)
        arrived(o_ref, n, pair_recv)


def solution(mesh):
    n = mesh.shape["sp"]

    def step(q, k, v):
        sequences, heads, head = q.shape
        tokens, kv = k.shape[1:3]
        share = heads // kv
        tall = tokens * kv
        group = tall // 8
        bf16, f32 = jnp.bfloat16, jnp.float32
        anywhere = pl.BlockSpec(memory_space=pl.ANY)
        dma = pltpu.SemaphoreType.DMA
        return pl.pallas_call(
            functools.partial(kernel, n, kv, share, head ** -0.5),
            out_shape=jax.ShapeDtypeStruct(q.shape, bf16),
            in_specs=[anywhere] * 3,
            out_specs=pl.BlockSpec(memory_space=pltpu.VMEM),
            scratch_shapes=[
                pltpu.VMEM((sequences, heads, head), bf16),
                pltpu.VMEM((SLOTS, tall, head), bf16),
                pltpu.VMEM((SLOTS, tall, head), bf16),
                pltpu.VMEM((group // 8, 8, LANES), f32),
                pltpu.VMEM((group // 8, 8, LANES), f32),
                pltpu.VMEM((LANES, group), bf16),
                pltpu.VMEM((LANES, group), bf16),
                pltpu.VMEM((sequences, heads, head), bf16),
                pltpu.VMEM((sequences, 1, LANES), f32),
                pltpu.VMEM((n + 1, 6, heads, head), bf16),
                pltpu.VMEM((n + 1, 6, 1, LANES), f32),
                pltpu.VMEM((n, n, heads, head), bf16),
                pltpu.VMEM((n, n, 1, LANES), f32),
                dma,
                dma((SLOTS,)),
                dma((SLOTS,)),
                dma,
                dma,
                dma,
                dma,
                dma((3,)),
                dma((3,)),
                dma((n // 2 + 1, n)),
                dma((2, n)),
                dma,
                dma((3,)),
                dma,
                dma,
                dma,
                dma,
            ],
            compiler_params=pltpu.CompilerParams(collective_id=0, has_side_effects=True, vmem_limit_bytes=56_000_000),
            name="decode",
        )(q, k.reshape(sequences, tall, head), v.reshape(sequences, tall, head))

    return jax.shard_map(
        step,
        mesh=mesh,
        in_specs=(P("dp", None, None), P("dp", "sp", None, None), P("dp", "sp", None, None)),
        out_specs=P("dp", None, None),
        check_vma=False,
    )
```
